32 devices in a mesh: gx: 4 (over x, core), gy: 4 (over z), gz: 2 (over y).
Axes of the slice: x: 2, y: 2, z: 4, core: 2. Of those that a mesh axis runs over, the one named last changes fastest.
Arguments:
- left_modes: bfloat16 [2, 4, 2, 128, 3, 16384], P(None, None, None, None, None, ('gx', 'gy', 'gz')), may hold values from -0.23925781 to 0.23925781
- right_modes: bfloat16 [2, 4, 2, 128, 3, 16384], P(None, None, None, None, None, ('gx', 'gy', 'gz')), may hold values from -0.23925781 to 0.23925781
- gamma_cols: int32 [16, 4], replicated, may hold values from 0 to 3, each once within a row
- gamma_phase: int32 [16, 4], replicated, may hold values from 0 to 3
- dilution: int32 [64], replicated, may hold values from 0 to 3
- time_pairs: int32 [4, 2], replicated, may hold values from 0 to 1
Outputs:
- meson_fields: float32 [16, 2, 2, 128, 128], P('gz', None, None, ('gx', 'gy'))
- traces: float32 [4, 16, 16, 2], P(None, 'gz')
The draws below stay inside these ranges and needn't reach their ends.
Inputs may be any that keep to these rules, and one draw needn't show every extreme that they name: Each row of gamma_cols is a permutation of the four spins.
All inputs are finite; a program needn't handle non-finite values.
Results may differ from the reference program's by a relative error of at most 0.0003.
Values sent between devices are 32-bit elements; how exact they have to be, the bound alone decides.
A program may use at most 128 MiB of HBM per device.

```python
import math
import jax
import jax.numpy as jnp
from jax import lax

LOW = 64
NOISE = 64
N = 128
G = 16
TS = 2
NPAIR = 4
SITES = 16384


def touch_ends(array, own_key, least, high):
    dims = array.shape
    index_at = [jax.random.randint(jax.random.fold_in(own_key, axis), (), 0, dims[axis]) for axis in range(len(dims))]
    array = array.at[tuple(index_at)].set(least)
    longest = dims.index(max(dims))
    index_at[longest] = (index_at[longest] + 1) % dims[longest]
    return array.at[tuple(index_at)].set(high)


def level_of(rng, shape, split, low, top_value):
    def one(dim, parts):
        draws = jax.random.uniform(jax.random.fold_in(jax.random.fold_in(rng, 6), dim), (parts,), jnp.float32, low / len(split), top_value / len(split))
        return jnp.repeat(jnp.exp(draws), shape[dim] // parts).reshape((-1,) + (1,) * (len(shape) - dim - 1))

    loudness = one(*split[0])
    for cut in split[1:]:
        loudness = loudness * one(*cut)
    return loudness


def noise(key, extent, spread, limit, shards=(), kind=jnp.bfloat16):
    values = spread * jax.random.normal(key, extent, jnp.float32)
    if shards:
        values = values * level_of(key, extent, shards, -0.22, 0.18)
    return jnp.clip(values, -limit, limit).astype(kind)


def setup_inputs(seed: int = 0) -> dict:
    key_list = jax.random.split(jax.random.key(seed), 7)
    return {
        "left_modes": noise(key_list[0], (TS, 4, 2, N, 3, SITES), ((24 * SITES) ** -0.25), 0.23925781, ((5, 32),)),
        "right_modes": noise(key_list[1], (TS, 4, 2, N, 3, SITES), ((24 * SITES) ** -0.25), 0.23925781, ((5, 32),)),
        "gamma_cols": jax.vmap(lambda own: jax.random.permutation(own, 4))(jax.random.split(key_list[2], G)).reshape((G, 4)).astype(jnp.int32),
        "gamma_phase": touch_ends(jax.random.randint(key_list[3], (G, 4), 0, 4), jax.random.fold_in(key_list[3], 1), 0, 3).astype(jnp.int32),
        "dilution": touch_ends(jax.random.randint(key_list[4], (NOISE,), 0, 4), jax.random.fold_in(key_list[4], 1), 0, 3).astype(jnp.int32),
        "time_pairs": touch_ends(jax.random.randint(key_list[5], (NPAIR, 2), 0, TS), jax.random.fold_in(key_list[5], 1), 0, TS - 1).astype(jnp.int32),
    }


EXACT = lax.Precision.HIGHEST


def pair_products(left_slice, right_slice):
    block_size = math.gcd(left_slice.shape[-1], 4096)
    block_count = left_slice.shape[-1] // block_size

    def add_block(block_index, running):
        offset = (block_index * block_size).astype(jnp.int32)
        left_part = lax.dynamic_slice_in_dim(left_slice, offset, block_size, 4).astype(jnp.float32)
        right_part = lax.dynamic_slice_in_dim(right_slice, offset, block_size, 4).astype(jnp.float32)
        return running + jnp.einsum("spicx,qrjcx->sqpirj", left_part, right_part, precision=EXACT)

    zero_total = jnp.zeros((4, 4, 2, N, 2, N), jnp.float32)
    products = lax.fori_loop(0, block_count, add_block, zero_total)
    pair_re = products[:, :, 0, :, 0, :] + products[:, :, 1, :, 1, :]
    pair_im = products[:, :, 0, :, 1, :] - products[:, :, 1, :, 0, :]
    return pair_re, pair_im


def coefficients(gamma_cols, gamma_phase):
    spin_ids = jnp.arange(4, dtype=jnp.int32)
    onehot = (gamma_cols[:, :, None] == spin_ids[None, None, :]).astype(jnp.float32)
    real_sign = (gamma_phase == 0).astype(jnp.float32) - (gamma_phase == 2).astype(jnp.float32)
    imag_sign = (gamma_phase == 1).astype(jnp.float32) - (gamma_phase == 3).astype(jnp.float32)
    return onehot * real_sign[:, :, None], onehot * imag_sign[:, :, None]


def spin_mask(dilution):
    noise_spin = jnp.concatenate([jnp.full((LOW,), -1, jnp.int32), dilution.astype(jnp.int32)])
    spin_ids = jnp.arange(4, dtype=jnp.int32)
    keep_spin = (noise_spin[None, :] < 0) | (noise_spin[None, :] == spin_ids[:, None])
    return keep_spin.astype(jnp.float32)


def select_pairs(crossed, time_pairs):
    time_ids = jnp.arange(crossed.shape[1], dtype=jnp.int32)
    first_time = (time_pairs[:, 0:1] == time_ids[None, :]).astype(jnp.float32)
    second_time = (time_pairs[:, 1:2] == time_ids[None, :]).astype(jnp.float32)
    chosen = jnp.einsum("pt,pu,gtahub->pgahb", first_time, second_time, crossed, precision=EXACT)
    real_part = chosen[:, :, 0, :, 0] - chosen[:, :, 1, :, 1]
    imag_part = chosen[:, :, 0, :, 1] + chosen[:, :, 1, :, 0]
    return jnp.stack([real_part, imag_part], axis=-1)


def reference(left_modes, right_modes, gamma_cols, gamma_phase, dilution, time_pairs):
    mask_table = spin_mask(dilution)
    coef_re, coef_im = coefficients(gamma_cols, gamma_phase)
    real_list = []
    imag_list = []
    for time_slot in range(TS):
        pair_re, pair_im = pair_products(left_modes[time_slot], right_modes[time_slot])
        real_list.append(pair_re * mask_table[None, :, None, :])
        imag_list.append(pair_im * mask_table[None, :, None, :])
    pair_re = jnp.stack(real_list)
    pair_im = jnp.stack(imag_list)
    meson_re = jnp.einsum("gst,ustij->guij", coef_re, pair_re, precision=EXACT) - jnp.einsum("gst,ustij->guij", coef_im, pair_im, precision=EXACT)
    meson_im = jnp.einsum("gst,ustij->guij", coef_re, pair_im, precision=EXACT) + jnp.einsum("gst,ustij->guij", coef_im, pair_re, precision=EXACT)
    meson_fields = jnp.stack([meson_re, meson_im], axis=2)
    crossed = jnp.einsum("gtaij,hubji->gtahub", meson_fields, meson_fields, precision=EXACT)
    traces = select_pairs(crossed, time_pairs) / N
    return meson_fields, traces
```

```python
import functools

import jax
import jax.numpy as jnp
from jax import lax
from jax.experimental import pallas as pl
from jax.experimental.pallas import tpu as pltpu
from jax.sharding import PartitionSpec as P

EXACT = lax.Precision.HIGHEST
MESH = pl.DeviceIdType.MESH
NT = (((1,), (1,)), ((), ()))


def nt_dot(a, b):
    return lax.dot_general(a, b, NT, preferred_element_type=jnp.float32)


def blocks_kernel(low, slabs, mask_ref, left_ref, right_ref, out_ref):
    spins = left_ref.shape[1]
    modes = left_ref.shape[4]
    depth = left_ref.shape[5]
    colour = pl.program_id(1)
    left_re = left_ref[0, :, 0, 0].reshape(spins * modes, depth)
    left_im = left_ref[0, :, 1, 0].reshape(spins * modes, depth)
    low_re = jnp.concatenate([right_ref[0, r, 0, 0, :low] for r in range(spins)], axis=0)
    low_im = jnp.concatenate([right_ref[0, r, 1, 0, :low] for r in range(spins)], axis=0)
    noise_re = right_ref[0, 0, 0, 0, low:] * mask_ref[0]
    noise_im = right_ref[0, 0, 1, 0, low:] * mask_ref[0]
    for r in range(1, spins):
        noise_re = noise_re + right_ref[0, r, 0, 0, low:] * mask_ref[r]
        noise_im = noise_im + right_ref[0, r, 1, 0, low:] * mask_ref[r]
    low_out_re = nt_dot(left_re, low_re) + nt_dot(left_im, low_im)
    low_out_im = nt_dot(left_re, low_im) + nt_dot(left_im, -low_re)
    noise_out = nt_dot(left_re, jnp.concatenate([noise_re, noise_im], axis=0)) + nt_dot(
        left_im, jnp.concatenate([noise_im, -noise_re], axis=0)
    )
    half = low_out_re.shape[1] // 128
    per_spin = 2 * half + 1

    pieces = []
    for s in range(spins):
        rows = slice(s * modes, (s + 1) * modes)
        for k in range(half):
            pieces.append((s * per_spin + k, low_out_re[rows, k * 128 : (k + 1) * 128]))
        for k in range(half):
            pieces.append((s * per_spin + half + k, low_out_im[rows, k * 128 : (k + 1) * 128]))
        pieces.append((s * per_spin + 2 * half, noise_out[rows]))

    @pl.when(colour == 0)
    def _():
        for k, piece in pieces:
            out_ref[0, k] = piece
        for k in range(len(pieces), slabs):
            out_ref[0, k] = jnp.zeros((modes, 128), jnp.float32)

    @pl.when(colour != 0)
    def _():
        for k, piece in pieces:
            out_ref[0, k] += piece


def local_blocks(left, right, dilution, slabs):
    times, spins, parts, colours, modes, depth = left.shape
    noise_count = dilution.shape[0]
    low = modes - noise_count
    mask = (dilution[None, :] == jnp.arange(spins, dtype=jnp.int32)[:, None]).astype(jnp.bfloat16)
    mask = jnp.broadcast_to(mask[:, :, None], (spins, noise_count, depth))
    block = (1, spins, parts, 1, modes, depth)
    return pl.pallas_call(
        functools.partial(blocks_kernel, low, slabs),
        grid=(times, colours),
        in_specs=[
            pl.BlockSpec((spins, noise_count, depth), lambda t, c: (0, 0, 0)),
            pl.BlockSpec(block, lambda t, c: (t, 0, 0, c, 0, 0)),
            pl.BlockSpec(block, lambda t, c: (t, 0, 0, c, 0, 0)),
        ],
        out_specs=pl.BlockSpec((1, slabs, modes, 128), lambda t, c: (t, 0, 0, 0)),
        out_shape=jax.ShapeDtypeStruct((times, slabs, modes, 128), jnp.float32),
        compiler_params=pltpu.CompilerParams(
            dimension_semantics=("arbitrary", "arbitrary"), vmem_limit_bytes=48 * 1024 * 1024
        ),
        name="spin_blocks",
    )(mask, left, right)


def chunk_transpose(rows, chunk):
    rows = list(rows)
    count = len(rows)
    lane = lax.broadcasted_iota(jnp.int32, rows[0].shape, 1) // chunk
    bit = 1
    while bit < count:
        upper = (lane // bit) % 2 == 1
        new = list(rows)
        for k in range(count):
            if k & bit:
                continue
            a, b = rows[k], rows[k | bit]
            new[k] = jnp.where(upper, pltpu.roll(b, bit * chunk, 1), a)
            new[k | bit] = jnp.where(upper, b, pltpu.roll(a, 128 - bit * chunk, 1))
        rows = new
        bit *= 2
    return rows


def exchange_kernel(
    dims, cols_ref, phase_ref, dil_ref, part_ref, meson_ref, trace_ref, *scratch
):
    (times, spins, low, gammas, gamma_local, nz, kz, nxo, nxi, ny, rows) = dims
    bufs = scratch[: 8 * times]
    (blocks, fields, outgoing, columns, totals, send_sem, recv_sem) = scratch[8 * times :]
    gx, gy, gz = lax.axis_index("gx"), lax.axis_index("gy"), lax.axis_index("gz")
    outer, inner = gx // nxi, gx % nxi
    nb = nxo * nxi * ny
    me = gx * ny + gy
    next_sem = [0]

    def block_peer(d):
        there = (me + d) % nb
        return there, {"gx": there // ny, "gy": there % ny, "gz": gz}

    barrier = pltpu.get_barrier_semaphore()
    for d in range(1, nb):
        _, device = block_peer(d)
        pl.semaphore_signal(barrier, inc=1, device_id=device, device_id_type=MESH)
    for d in range(1, nz):
        pl.semaphore_signal(
            barrier, inc=1, device_id={"gx": gx, "gy": gy, "gz": (gz + d) % nz}, device_id_type=MESH
        )
    pl.semaphore_wait(barrier, nb - 1 + nz - 1)

    def send(src, dst, device):
        k = next_sem[0]
        next_sem[0] += 1
        copy = pltpu.make_async_remote_copy(
            src_ref=src, dst_ref=dst, send_sem=send_sem.at[k], recv_sem=recv_sem.at[k],
            device_id=device, device_id_type=MESH,
        )
        copy.start()
        return copy

    def peer(axis, d):
        if axis == "inner":
            there = (inner + d) % nxi
            return there, {"gx": outer * nxi + there, "gy": gy, "gz": gz}
        if axis == "outer":
            there = (outer + d) % nxo
            return there, {"gx": there * nxi + inner, "gy": gy, "gz": gz}
        if axis == "gy":
            there = (gy + d) % ny
            return there, {"gx": gx, "gy": there, "gz": gz}
        there = (gz + d) % nz
        return there, {"gx": gx, "gy": gy, "gz": there}

    place = {"inner": inner, "outer": outer, "gy": gy, "gz": gz}
    size = {"inner": nxi, "outer": nxo, "gy": ny, "gz": nz}
    full = ["gz", "kz", "outer", "inner", "gy"]

    def begin(src, labels, axis, arrivals):
        at = labels.index(axis)
        copies = []
        for d in range(1, size[axis]):
            there, device = peer(axis, d)
            index = (slice(None),) * at + (there,)
            copies.append(send(src.at[index], arrivals.at[d - 1], device))
        return copies

    def finish(copies, src, labels, axis, arrivals, result):
        at = labels.index(axis)
        total = src[(slice(None),) * at + (place[axis],)]
        for d, copy in enumerate(copies):
            copy.wait_recv()
            total = total + arrivals[d]
        result[...] = total
        return [label for label in labels if label != axis]

    flows = []
    for t in range(times):
        order = ["inner", "outer", "gz", "gy"] if t % 2 == 0 else ["inner", "gz", "outer", "gy"]
        flows.append({"order": order, "src": part_ref.at[t], "labels": full, "bufs": bufs[8 * t : 8 * t + 8]})
    pending = []
    for step in range(4):
        for flow in flows:
            if step > 0:
                flow["labels"] = finish(
                    flow["copies"], flow["src"], flow["labels"], flow["order"][step - 1],
                    flow["bufs"][2 * step - 2], flow["bufs"][2 * step - 1],
                )
                flow["src"] = flow["bufs"][2 * step - 1]
            flow["copies"] = begin(flow["src"], flow["labels"], flow["order"][step], flow["bufs"][2 * step])
            pending += flow["copies"]
    for t, flow in enumerate(flows):
        finish(flow["copies"], flow["src"], flow["labels"], "gy", flow["bufs"][6], flow["bufs"][7].at[gz])
        mine = flow["bufs"][7].at[gz]
        flow["copies"] = [send(mine, flow["bufs"][7].at[gz], peer("gz", d)[1]) for d in range(1, nz)]
        pending += flow["copies"]

    half = spins * low // 128
    per_spin = 2 * half + 1
    lane = lax.broadcasted_iota(jnp.int32, (rows, 128), 1)
    is_low = lane < low
    dil = jnp.broadcast_to(dil_ref[...], (rows, 128))
    pack = 128 // low

    for t, flow in enumerate(flows):
        for copy in flow["copies"]:
            copy.wait_recv()
        own = flow["bufs"][7]

        def slab(k):
            return own[k // kz, k % kz]

        for s in range(spins):
            noise = slab(s * per_spin + 2 * half)
            for c in range(2):
                noise_c = noise if c == 1 else pltpu.roll(noise, low, 1)
                for r in range(spins):
                    piece = slab(s * per_spin + c * half + r // pack)
                    if r % pack:
                        piece = pltpu.roll(piece, 128 - (r % pack) * low, 1)
                    blocks[t, s, r, c] = jnp.where(
                        is_low, piece, jnp.where(dil == r, noise_c, 0.0)
                    )

    def one_gamma(g, carry):
        for t in range(times):
            re = jnp.zeros((rows, 128), jnp.float32)
            im = jnp.zeros((rows, 128), jnp.float32)
            for s in range(spins):
                col = cols_ref[g, s]
                phase = phase_ref[g, s]
                block_re = blocks[t, s, col, 0]
                block_im = blocks[t, s, col, 1]
                one = jnp.where(phase == 0, 1.0, jnp.where(phase == 2, -1.0, 0.0))
                eye = jnp.where(phase == 1, 1.0, jnp.where(phase == 3, -1.0, 0.0))
                re = re + (one * block_re - eye * block_im)
                im = im + (one * block_im + eye * block_re)
            fields[t, 0, g] = re
            fields[t, 1, g] = im
        return carry

    lax.fori_loop(0, gammas, one_gamma, 0)

    picked = []
    for t in range(times):
        for c in range(2):
            for g in range(gamma_local):
                value = fields[t, c, gz * gamma_local + g]
                meson_ref[g, t, c] = value
                picked.append(value)
    while len(picked) % nb:
        picked.append(jnp.zeros((rows, 128), jnp.float32))
    groups = len(picked) // nb
    for k in range(groups):
        moved = chunk_transpose(picked[k * nb : (k + 1) * nb], rows)
        for j in range(nb):
            outgoing[j, :, k * 128 : (k + 1) * 128] = moved[j]
    columns[me] = outgoing[me]
    copies = []
    for d in range(1, nb):
        there, device = block_peer(d)
        copies.append(send(outgoing.at[there], columns.at[me], device))
    pending += copies
    for copy in copies:
        copy.wait_recv()
    width = groups * 128
    right = columns[...].reshape(nb * rows, width)
    quarter = gammas * rows
    count = times * 2 * gamma_local
    lane_w = lax.broadcasted_iota(jnp.int32, (quarter, width), 1)
    row_w = lax.broadcasted_iota(jnp.int32, (quarter, width), 0)
    same = (row_w % rows) == (lane_w % rows)
    pick_from = lax.broadcasted_iota(jnp.int32, (width, 128), 0) // rows
    pick_to = lax.broadcasted_iota(jnp.int32, (width, 128), 1)
    partial = jnp.zeros((gammas, 128), jnp.float32)
    for t in range(times):
        for c in range(2):
            q = t * 2 + c
            left = fields[t, c].reshape(quarter, 128)
            cross = jnp.dot(left, right, precision=EXACT, preferred_element_type=jnp.float32)
            cross = jnp.where(same, cross, 0.0)
            cross = jnp.sum(cross.reshape(gammas, rows, width), axis=1)
            pick = ((pick_to == pick_from + q * count) & (pick_from < count)).astype(jnp.float32)
            partial = partial + jnp.dot(cross, pick, precision=EXACT, preferred_element_type=jnp.float32)
    totals[me] = partial
    copies = []
    for d in range(1, nb):
        _, device = block_peer(d)
        copies.append(send(totals.at[me], totals.at[me], device))
    pending += copies
    for copy in copies:
        copy.wait_recv()
    total = totals[0]
    for j in range(1, nb):
        total = total + totals[j]
    trace_ref[...] = total
    for copy in pending:
        copy.wait_send()


def exchange(parts, gamma_cols, gamma_phase, dilution, sizes, modes):
    nx, ny, nz = sizes
    times, slabs = parts.shape[:2]
    nxi = 2 if nx % 2 == 0 else 1
    nxo = nx // nxi
    kz = slabs // nz
    gammas, spins = gamma_cols.shape
    gamma_local = gammas // nz
    low = modes - dilution.shape[0]
    rows = modes // (nx * ny)
    nb = nx * ny
    parts = parts.reshape(times, nz, kz, nxo, nxi, ny, rows, 128)
    tile = (rows, 128)
    dil = jnp.concatenate([jnp.full((low,), -1, jnp.int32), dilution]).reshape(1, modes)
    dims = (times, spins, low, gammas, gamma_local, nz, kz, nxo, nxi, ny, rows)
    scratch = []
    sems = 0
    for t in range(times):
        shapes = []
        left_dims = {"gz": nz, "kz": kz, "outer": nxo, "inner": nxi, "gy": ny}
        order = ["inner", "outer", "gz", "gy"] if t % 2 == 0 else ["inner", "gz", "outer", "gy"]
        for axis in order:
            n = left_dims.pop(axis)
            sems += n - 1
            rest = tuple(left_dims.values())
            shapes.append((max(n - 1, 1),) + rest + tile)
            shapes.append(rest + tile)
        shapes[-1] = (nz, kz) + tile
        sems += nz - 1
        scratch += [pltpu.VMEM(shape, jnp.float32) for shape in shapes]
    sems += 2 * (nb - 1)
    groups = -(-(times * 2 * gamma_local) // nb)
    scratch += [
        pltpu.VMEM((times, spins, spins, 2) + tile, jnp.float32),
        pltpu.VMEM((times, 2, gammas) + tile, jnp.float32),
        pltpu.VMEM((nb, rows, groups * 128), jnp.float32),
        pltpu.VMEM((nb, rows, groups * 128), jnp.float32),
        pltpu.VMEM((nb, gammas, 128), jnp.float32),
        pltpu.SemaphoreType.DMA((sems,)),
        pltpu.SemaphoreType.DMA((sems,)),
    ]
    vmem = pl.BlockSpec(memory_space=pltpu.VMEM)
    smem = pl.BlockSpec(memory_space=pltpu.SMEM)
    return pl.pallas_call(
        functools.partial(exchange_kernel, dims),
        in_specs=[smem, smem, vmem, vmem],
        out_specs=[vmem, vmem],
        out_shape=[
            jax.ShapeDtypeStruct((gamma_local, times, 2) + tile, jnp.float32),
            jax.ShapeDtypeStruct((gammas, 128), jnp.float32),
        ],
        scratch_shapes=scratch,
        compiler_params=pltpu.CompilerParams(
            collective_id=0, has_side_effects=True, vmem_limit_bytes=48 * 1024 * 1024
        ),
        name="exchange",
    )(gamma_cols, gamma_phase, dil, parts)


def local(sizes, left_modes, right_modes, gamma_cols, gamma_phase, dilution, time_pairs):
    left = jnp.transpose(left_modes, (0, 1, 2, 4, 3, 5))
    right = jnp.transpose(right_modes, (0, 1, 2, 4, 3, 5))
    times, spins = left.shape[:2]
    modes = left.shape[4]
    noise_count = dilution.shape[0]
    low = modes - noise_count
    nz = sizes[2]
    used = spins * (2 * (spins * low // 128) + 1)
    slabs = -(-used // nz) * nz
    parts = local_blocks(left, right, dilution, slabs)
    meson_fields, packed = exchange(parts, gamma_cols, gamma_phase, dilution, sizes, modes)
    gammas = gamma_cols.shape[0]
    gamma_local = gammas // nz
    grid = packed[:, : times * 2 * times * 2 * gamma_local]
    grid = grid.reshape(gammas, times, 2, times, 2, gamma_local)
    time_ids = jnp.arange(times, dtype=jnp.int32)
    first = time_pairs[:, 0:1] == time_ids[None, :]
    second = time_pairs[:, 1:2] == time_ids[None, :]
    keep = first[:, None, :] & second[:, :, None]
    real = grid[:, :, 0, :, 0] - grid[:, :, 1, :, 1]
    imag = grid[:, :, 1, :, 0] + grid[:, :, 0, :, 1]
    both = jnp.stack([real, imag], axis=-1)
    chosen = jnp.where(keep[:, None, :, :, None, None], both[None], 0.0)
    traces = jnp.transpose(jnp.sum(chosen, axis=(2, 3)), (0, 2, 1, 3)) / modes
    return (meson_fields, traces)


def solution(mesh):
    sizes = (mesh.shape["gx"], mesh.shape["gy"], mesh.shape["gz"])
    modes_spec = P(None, None, None, None, None, ("gx", "gy", "gz"))
    return jax.shard_map(
        functools.partial(local, sizes),
        mesh=mesh,
        in_specs=(modes_spec, modes_spec, P(), P(), P(), P()),
        out_specs=(P("gz", None, None, ("gx", "gy"), None), P(None, "gz", None, None)),
        check_vma=False,
    )
```

```python
import functools

import jax
import jax.numpy as jnp
from jax import lax
from jax.experimental import pallas as pl
from jax.experimental.pallas import tpu as pltpu
from jax.sharding import PartitionSpec as P

EXACT = lax.Precision.HIGHEST
MESH = pl.DeviceIdType.MESH
NT = (((1,), (1,)), ((), ()))


def nt_dot(a, b):
    return lax.dot_general(a, b, NT, preferred_element_type=jnp.float32)


def chunk_transpose(rows, chunk):
    rows = list(rows)
    count = len(rows)
    lane = lax.broadcasted_iota(jnp.int32, rows[0].shape, 1) // chunk
    bit = 1
    while bit < count:
        upper = (lane // bit) % 2 == 1
        new = list(rows)
        for k in range(count):
            if k & bit:
                continue
            a, b = rows[k], rows[k | bit]
            new[k] = jnp.where(upper, pltpu.roll(b, bit * chunk, 1), a)
            new[k | bit] = jnp.where(upper, b, pltpu.roll(a, 128 - bit * chunk, 1))
        rows = new
        bit *= 2
    return rows


def flow_list(times):
    flows = []
    for t in range(times):
        flows.append((t, 0, ("inner", "outer", "gz", "gy")))
        flows.append((t, 1, ("inner", "gz", "outer", "gy")))
    return flows


def slab_range(part, kz):
    cut = kz // 2
    return (0, cut) if part == 0 else (cut, kz)


def fused_kernel(
    dims, cols_ref, phase_ref, dil_ref, left_ref, right_ref, meson_ref, trace_ref, *scratch
):
    (times, spins, colours, low, modes, depth, gammas, gamma_local, nz, kz, nxo, nxi, ny, rows) = dims
    flow_specs = flow_list(times)
    bufs = scratch[: 7 * len(flow_specs)]
    (
        left_buf, right_buf, parts, gathered, blocks, fields, outgoing, columns, totals,
        load_sem, send_sem, recv_sem,
    ) = scratch[7 * len(flow_specs) :]
    gx, gy, gz = lax.axis_index("gx"), lax.axis_index("gy"), lax.axis_index("gz")
    outer, inner = gx // nxi, gx % nxi
    nb = nxo * nxi * ny
    me = gx * ny + gy
    next_sem = [0]

    loads = []
    for t in range(times):
        for colour in range(colours):
            k = 2 * (t * colours + colour)
            pair = (
                pltpu.make_async_copy(
                    right_ref.at[t, :, :, colour], right_buf.at[t, colour], load_sem.at[k]
                ),
                pltpu.make_async_copy(
                    left_ref.at[t, :, :, colour], left_buf.at[t, colour], load_sem.at[k + 1]
                ),
            )
            for copy in pair:
                copy.start()
            loads.append(pair)

    def block_peer(d):
        there = (me + d) % nb
        return there, {"gx": there // ny, "gy": there % ny, "gz": gz}

    barrier = pltpu.get_barrier_semaphore()
    for d in range(1, nb):
        _, device = block_peer(d)
        pl.semaphore_signal(barrier, inc=1, device_id=device, device_id_type=MESH)
    for d in range(1, nz):
        pl.semaphore_signal(
            barrier, inc=1, device_id={"gx": gx, "gy": gy, "gz": (gz + d) % nz}, device_id_type=MESH
        )

    noise_count = modes - low
    at_lane = lax.broadcasted_iota(jnp.int32, (noise_count, modes), 1)
    at_row = lax.broadcasted_iota(jnp.int32, (noise_count, modes), 0)
    dil_row = jnp.broadcast_to(dil_ref[...], (noise_count, modes))
    masks = []
    for r in range(spins):
        hit = jnp.where((at_lane == at_row + low) & (dil_row == r), 1.0, 0.0)
        column = jnp.sum(hit, axis=1, keepdims=True)
        masks.append(jnp.broadcast_to(column, (noise_count, depth)).astype(jnp.bfloat16))

    half = spins * low // 128
    per_spin = 2 * half + 1

    def multiply(t, colour):
        for copy in loads[t * colours + colour]:
            copy.wait()
        left = left_buf.at[t, colour]
        right = right_buf.at[t, colour]
        left_re = left[:, 0].reshape(spins * modes, depth)
        left_im = left[:, 1].reshape(spins * modes, depth)
        low_re = jnp.concatenate([right[r, 0, :low] for r in range(spins)], axis=0)
        low_im = jnp.concatenate([right[r, 1, :low] for r in range(spins)], axis=0)
        noise_re = right[0, 0, low:] * masks[0]
        noise_im = right[0, 1, low:] * masks[0]
        for r in range(1, spins):
            noise_re = noise_re + right[r, 0, low:] * masks[r]
            noise_im = noise_im + right[r, 1, low:] * masks[r]
        low_out_re = nt_dot(left_re, low_re) + nt_dot(left_im, low_im)
        low_out_im = nt_dot(left_re, low_im) + nt_dot(left_im, -low_re)
        noise_out = nt_dot(left_re, jnp.concatenate([noise_re, noise_im], axis=0)) + nt_dot(
            left_im, jnp.concatenate([noise_im, -noise_re], axis=0)
        )

        def put(k, piece):
            piece = piece.reshape(nxo, nxi, ny, rows, 128)
            if colour == 0:
                parts[t, k // kz, k % kz] = piece
            else:
                parts[t, k // kz, k % kz] += piece

        for s in range(spins):
            at = slice(s * modes, (s + 1) * modes)
            for k in range(half):
                put(s * per_spin + k, low_out_re[at, k * 128 : (k + 1) * 128])
                put(s * per_spin + half + k, low_out_im[at, k * 128 : (k + 1) * 128])
            put(s * per_spin + 2 * half, noise_out[at])
        if colour == 0:
            for k in range(spins * per_spin, nz * kz):
                parts[t, k // kz, k % kz] = jnp.zeros((nxo, nxi, ny, rows, 128), jnp.float32)

    pending = []

    def send(src, dst, device):
        k = next_sem[0]
        next_sem[0] += 1
        copy = pltpu.make_async_remote_copy(
            src_ref=src, dst_ref=dst, send_sem=send_sem.at[k], recv_sem=recv_sem.at[k],
            device_id=device, device_id_type=MESH,
        )
        copy.start()
        pending.append(copy)
        return copy

    def peer(axis, d):
        if axis == "inner":
            there = (inner + d) % nxi
            return there, {"gx": outer * nxi + there, "gy": gy, "gz": gz}
        if axis == "outer":
            there = (outer + d) % nxo
            return there, {"gx": there * nxi + inner, "gy": gy, "gz": gz}
        if axis == "gy":
            there = (gy + d) % ny
            return there, {"gx": gx, "gy": there, "gz": gz}
        there = (gz + d) % nz
        return there, {"gx": gx, "gy": gy, "gz": there}

    place = {"inner": inner, "outer": outer, "gy": gy, "gz": gz}
    size = {"inner": nxi, "outer": nxo, "gy": ny, "gz": nz}

    def begin(flow):
        axis = flow["order"][flow["step"]]
        at = flow["labels"].index(axis)
        arrivals = flow["bufs"][2 * flow["step"]]
        flow["copies"] = []
        for d in range(1, size[axis]):
            there, device = peer(axis, d)
            index = (slice(None),) * at + (there,)
            flow["copies"].append(send(flow["src"].at[index], arrivals.at[d - 1], device))

    def finish(flow):
        step = flow["step"]
        axis = flow["order"][step]
        at = flow["labels"].index(axis)
        arrivals = flow["bufs"][2 * step]
        total = flow["src"][(slice(None),) * at + (place[axis],)]
        for d, copy in enumerate(flow["copies"]):
            copy.wait_recv()
            total = total + arrivals[d]
        if step < 3:
            result = flow["bufs"][2 * step + 1]
        else:
            result = gathered.at[flow["t"], gz, flow["k0"] : flow["k1"]]
        result[...] = total
        flow["src"] = result
        flow["labels"] = [label for label in flow["labels"] if label != axis]
        flow["step"] = step + 1

    flows = []
    for n, (t, part, order) in enumerate(flow_specs):
        k0, k1 = slab_range(part, kz)
        flows.append({
            "t": t, "k0": k0, "k1": k1, "order": order, "step": 0,
            "src": parts.at[t, :, k0:k1],
            "labels": ["gz", "kz", "outer", "inner", "gy"],
            "bufs": bufs[7 * n : 7 * n + 7],
        })

    def advance(t):
        for flow in flows:
            if flow["t"] != t:
                continue
            if "copies" in flow and flow["step"] < 4:
                finish(flow)
            if flow["step"] < 4:
                begin(flow)
            else:
                mine = gathered.at[t, gz, flow["k0"] : flow["k1"]]
                flow["copies"] = [send(mine, mine, peer("gz", d)[1]) for d in range(1, nz)]

    lane = lax.broadcasted_iota(jnp.int32, (rows, 128), 1)
    is_low = lane < low
    dil = jnp.broadcast_to(dil_ref[...], (rows, 128))
    pack = 128 // low
    groups = -(-(2 * gamma_local) // nb)
    width = groups * 128

    def make_fields(t):
        for flow in flows:
            if flow["t"] == t:
                for copy in flow["copies"]:
                    copy.wait_recv()

        def slab(k):
            return gathered[t, k // kz, k % kz]

        for s in range(spins):
            noise = slab(s * per_spin + 2 * half)
            for c in range(2):
                noise_c = noise if c == 1 else pltpu.roll(noise, low, 1)
                for r in range(spins):
                    piece = slab(s * per_spin + c * half + r // pack)
                    if r % pack:
                        piece = pltpu.roll(piece, 128 - (r % pack) * low, 1)
                    blocks[t, s, r, c] = jnp.where(
                        is_low, piece, jnp.where(dil == r, noise_c, 0.0)
                    )

        def one_gamma(g, carry):
            re = jnp.zeros((rows, 128), jnp.float32)
            im = jnp.zeros((rows, 128), jnp.float32)
            for s in range(spins):
                col = cols_ref[g, s]
                phase = phase_ref[g, s]
                block_re = blocks[t, s, col, 0]
                block_im = blocks[t, s, col, 1]
                one = jnp.where(phase == 0, 1.0, jnp.where(phase == 2, -1.0, 0.0))
                eye = jnp.where(phase == 1, 1.0, jnp.where(phase == 3, -1.0, 0.0))
                re = re + (one * block_re - eye * block_im)
                im = im + (one * block_im + eye * block_re)
            fields[t, 0, g] = re
            fields[t, 1, g] = im
            return carry

        lax.fori_loop(0, gammas, one_gamma, 0)

    def send_columns(t):
        picked = []
        for c in range(2):
            for g in range(gamma_local):
                value = fields[t, c, gz * gamma_local + g]
                meson_ref[g, t, c] = value
                picked.append(value)
        while len(picked) % nb:
            picked.append(jnp.zeros((rows, 128), jnp.float32))
        for k in range(groups):
            moved = chunk_transpose(picked[k * nb : (k + 1) * nb], rows)
            for j in range(nb):
                outgoing[t, j, :, k * 128 : (k + 1) * 128] = moved[j]
        columns[t, me] = outgoing[t, me]
        copies = []
        for d in range(1, nb):
            there, device = block_peer(d)
            copies.append(send(outgoing.at[t, there], columns.at[t, me], device))
        return copies

    for colour in range(colours):
        multiply(0, colour)
    pl.semaphore_wait(barrier, nb - 1 + nz - 1)
    advance(0)
    for t in range(1, times):
        for colour in range(colours):
            multiply(t, colour)
            if t == 1 and colour == 0:
                advance(0)
        advance(t)
    done = {0: 2}
    for t in range(1, times):
        done[t] = 1
    arriving = {}
    while len(arriving) < times:
        for t in range(times):
            if done[t] < 5:
                advance(t)
                done[t] += 1
            elif t not in arriving:
                make_fields(t)
                arriving[t] = send_columns(t)

    quarter = gammas * rows
    wide = times * width
    rights = []
    for t in range(times):
        for copy in arriving[t]:
            copy.wait_recv()
        rights.append(columns[t].reshape(nb * rows, width))
    right = jnp.concatenate(rights, axis=1)
    row_w = lax.broadcasted_iota(jnp.int32, (quarter, wide), 0)
    lane_w = lax.broadcasted_iota(jnp.int32, (quarter, wide), 1)
    same = (row_w % rows) == (lane_w % rows)
    per = times * 2 * gamma_local
    src_lane = lax.broadcasted_iota(jnp.int32, (wide, 128), 0)
    dst = lax.broadcasted_iota(jnp.int32, (wide, 128), 1) % per
    src_t = src_lane // width
    src_x = (src_lane % width) // rows
    dst_t = dst // (2 * gamma_local)
    dst_x = dst % (2 * gamma_local)
    swapped = (dst_x + gamma_local) % (2 * gamma_local)
    same_t = src_t == dst_t
    straight = jnp.where(same_t & (src_x == dst_x), 1.0, 0.0)
    crossed = jnp.where(
        same_t & (src_x == swapped), jnp.where(dst_x < gamma_local, -1.0, 1.0), 0.0
    )
    picks = (straight, crossed)
    split = max(1, 128 // (per * times))
    while gammas % split or (gammas // split) % 8:
        split -= 1
    part_rows = gammas // split
    out_lane = lax.broadcasted_iota(jnp.int32, (part_rows, 128), 1) // per
    packed = jnp.zeros((part_rows, 128), jnp.float32)
    sums = [[None] * times, [None] * times]
    for t in range(times):
        for c in range(2):
            left = fields[t, c].reshape(quarter, 128)
            cross = jnp.dot(left, right, precision=EXACT, preferred_element_type=jnp.float32)
            cross = jnp.where(same, cross, 0.0)
            sums[c][t] = jnp.sum(cross.reshape(gammas, rows, wide), axis=1)
    total = jnp.dot(
        jnp.concatenate(sums[0], axis=0), straight, precision=EXACT,
        preferred_element_type=jnp.float32,
    ) + jnp.dot(
        jnp.concatenate(sums[1], axis=0), crossed, precision=EXACT,
        preferred_element_type=jnp.float32,
    )
    for t in range(times):
        for h in range(split):
            piece = total[t * gammas + h * part_rows : t * gammas + (h + 1) * part_rows]
            packed = jnp.where(out_lane == h * times + t, piece, packed)
    totals[me] = packed
    copies = []
    for d in range(1, nb):
        _, device = block_peer(d)
        copies.append(send(totals.at[me], totals.at[me], device))
    for copy in copies:
        copy.wait_recv()
    total = totals[0]
    for j in range(1, nb):
        total = total + totals[j]
    trace_ref[...] = total
    for copy in pending:
        copy.wait_send()


def fused(left, right, gamma_cols, gamma_phase, dilution, sizes):
    nx, ny, nz = sizes
    times, spins, parts, colours, modes, depth = left.shape
    nxi = 2 if nx % 2 == 0 else 1
    nxo = nx // nxi
    gammas = gamma_cols.shape[0]
    gamma_local = gammas // nz
    low = modes - dilution.shape[0]
    used = spins * (2 * (spins * low // 128) + 1)
    kz = -(-used // nz)
    rows = modes // (nx * ny)
    nb = nx * ny
    tile = (rows, 128)
    dil = jnp.concatenate([jnp.full((low,), -1, jnp.int32), dilution]).reshape(1, modes)
    dims = (
        times, spins, colours, low, modes, depth, gammas, gamma_local, nz, kz, nxo, nxi, ny, rows,
    )
    scratch = []
    sems = 0
    for t, part, order in flow_list(times):
        k0, k1 = slab_range(part, kz)
        shapes = []
        left_dims = {"gz": nz, "kz": k1 - k0, "outer": nxo, "inner": nxi, "gy": ny}
        for axis in order:
            n = left_dims.pop(axis)
            sems += n - 1
            rest = tuple(left_dims.values())
            shapes.append((max(n - 1, 1),) + rest + tile)
            shapes.append(rest + tile)
        sems += nz - 1
        scratch += [pltpu.VMEM(shape, jnp.float32) for shape in shapes[:7]]
    sems += (times + 1) * (nb - 1)
    groups = -(-(2 * gamma_local) // nb)
    per = times * 2 * gamma_local
    split = max(1, 128 // (per * times))
    while gammas % split or (gammas // split) % 8:
        split -= 1
    block = (times, colours, spins, parts, modes, depth)
    scratch += [
        pltpu.VMEM(block, jnp.bfloat16),
        pltpu.VMEM(block, jnp.bfloat16),
        pltpu.VMEM((times, nz, kz, nxo, nxi, ny) + tile, jnp.float32),
        pltpu.VMEM((times, nz, kz) + tile, jnp.float32),
        pltpu.VMEM((times, spins, spins, 2) + tile, jnp.float32),
        pltpu.VMEM((times, 2, gammas) + tile, jnp.float32),
        pltpu.VMEM((times, nb, rows, groups * 128), jnp.float32),
        pltpu.VMEM((times, nb, rows, groups * 128), jnp.float32),
        pltpu.VMEM((nb, gammas // split, 128), jnp.float32),
        pltpu.SemaphoreType.DMA((2 * times * colours,)),
        pltpu.SemaphoreType.DMA((sems,)),
        pltpu.SemaphoreType.DMA((sems,)),
    ]
    vmem = pl.BlockSpec(memory_space=pltpu.VMEM)
    smem = pl.BlockSpec(memory_space=pltpu.SMEM)
    hbm = pl.BlockSpec(memory_space=pl.ANY)
    meson, packed = pl.pallas_call(
        functools.partial(fused_kernel, dims),
        in_specs=[smem, smem, vmem, hbm, hbm],
        out_specs=[vmem, vmem],
        out_shape=[
            jax.ShapeDtypeStruct((gamma_local, times, 2) + tile, jnp.float32),
            jax.ShapeDtypeStruct((gammas // split, 128), jnp.float32),
        ],
        scratch_shapes=scratch,
        compiler_params=pltpu.CompilerParams(
            collective_id=0, has_side_effects=True, vmem_limit_bytes=60 * 1024 * 1024
        ),
        name="meson_fields",
    )(gamma_cols, gamma_phase, dil, left, right)
    grid = packed[:, : split * times * per]
    grid = grid.reshape(gammas // split, split, times, times, 2, gamma_local)
    return meson, jnp.transpose(grid, (2, 3, 5, 1, 0, 4)).reshape(
        times, times, gamma_local, gammas, 2
    )


def local(sizes, left_modes, right_modes, gamma_cols, gamma_phase, dilution, time_pairs):
    left = jnp.transpose(left_modes, (0, 1, 2, 4, 3, 5))
    right = jnp.transpose(right_modes, (0, 1, 2, 4, 3, 5))
    times = left.shape[0]
    modes = left.shape[4]
    meson_fields, grid = fused(left, right, gamma_cols, gamma_phase, dilution, sizes)
    time_ids = jnp.arange(times, dtype=jnp.int32)
    first = time_pairs[:, 0:1] == time_ids[None, :]
    second = time_pairs[:, 1:2] == time_ids[None, :]
    keep = second[:, :, None] & first[:, None, :]
    chosen = jnp.where(keep[:, :, :, None, None, None], grid[None], 0.0)
    traces = jnp.sum(chosen, axis=(1, 2)) / modes
    return (meson_fields, traces)


def solution(mesh):
    sizes = (mesh.shape["gx"], mesh.shape["gy"], mesh.shape["gz"])
    modes_spec = P(None, None, None, None, None, ("gx", "gy", "gz"))
    return jax.shard_map(
        functools.partial(local, sizes),
        mesh=mesh,
        in_specs=(modes_spec, modes_spec, P(), P(), P(), P()),
        out_specs=(P("gz", None, None, ("gx", "gy"), None), P(None, "gz", None, None)),
        check_vma=False,
    )
```

```python
import functools

import jax
import jax.numpy as jnp
from jax import lax
from jax.experimental import pallas as pl
from jax.experimental.pallas import tpu as pltpu
from jax.sharding import PartitionSpec as P

EXACT = lax.Precision.HIGHEST
MESH = pl.DeviceIdType.MESH
NT = (((1,), (1,)), ((), ()))


TAIL = 5
CUTS0 = (0, 1, 3)
CUTS1 = (0, 1, 3)


def nt_dot(a, b):
    return lax.dot_general(a, b, NT, preferred_element_type=jnp.float32)


def chunk_transpose(rows, chunk):
    rows = list(rows)
    count = len(rows)
    lane = lax.broadcasted_iota(jnp.int32, rows[0].shape, 1) // chunk
    bit = 1
    while bit < count:
        upper = (lane // bit) % 2 == 1
        new = list(rows)
        for k in range(count):
            if k & bit:
                continue
            a, b = rows[k], rows[k | bit]
            new[k] = jnp.where(upper, pltpu.roll(b, bit * chunk, 1), a)
            new[k | bit] = jnp.where(upper, b, pltpu.roll(a, 128 - bit * chunk, 1))
        rows = new
        bit *= 2
    return rows


def flow_list(times, kz):
    tail = kz // TAIL if TAIL else 0
    cut = (kz - tail + 1) // 2
    orders = (
        (0, cut, ("inner", "outer", "gz", "gy")),
        (cut, kz - tail, ("inner", "gz", "outer", "gy")),
        (kz - tail, kz, ("inner", "gy", "outer", "gz")),
    )
    return [(t,) + flow for t in range(times) for flow in orders if flow[0] < flow[1]]


def fused_kernel(
    dims, cols_ref, phase_ref, pairs_ref, dil_ref, left_ref, right_ref, meson_ref, trace_ref, *scratch
):
    (times, spins, colours, low, modes, depth, gammas, gamma_local, nz, kz, nxo, nxi, ny, rows) = dims
    flow_specs = flow_list(times, kz)
    bufs = scratch[: 7 * len(flow_specs)]
    (
        left_buf, right_buf, parts, gathered, blocks, fields, outgoing, columns, totals,
        load_sem, send_sem, recv_sem,
    ) = scratch[7 * len(flow_specs) :]
    gx, gy, gz = lax.axis_index("gx"), lax.axis_index("gy"), lax.axis_index("gz")
    outer, inner = gx // nxi, gx % nxi
    nb = nxo * nxi * ny
    me = gx * ny + gy
    next_sem = [0]

    loads = []
    for t in range(times):
        for colour in range(colours):
            k = 2 * (t * colours + colour)
            pair = (
                pltpu.make_async_copy(
                    right_ref.at[t, :, :, colour], right_buf.at[t, colour], load_sem.at[k]
                ),
                pltpu.make_async_copy(
                    left_ref.at[t, :, :, colour], left_buf.at[t, colour], load_sem.at[k + 1]
                ),
            )
            for copy in pair:
                copy.start()
            loads.append(pair)

    def block_peer(d):
        there = (me + d) % nb
        return there, {"gx": there // ny, "gy": there % ny, "gz": gz}

    barrier = pltpu.get_barrier_semaphore()
    for d in range(1, nb):
        _, device = block_peer(d)
        pl.semaphore_signal(barrier, inc=1, device_id=device, device_id_type=MESH)
    for d in range(1, nz):
        pl.semaphore_signal(
            barrier, inc=1, device_id={"gx": gx, "gy": gy, "gz": (gz + d) % nz}, device_id_type=MESH
        )

    noise_count = modes - low
    at_lane = lax.broadcasted_iota(jnp.int32, (noise_count, noise_count), 1)
    at_row = lax.broadcasted_iota(jnp.int32, (noise_count, noise_count), 0)
    dil_row = jnp.broadcast_to(dil_ref[...], (noise_count, noise_count)).astype(jnp.float32)
    dil_col = jnp.sum(jnp.where(at_lane == at_row, dil_row, 0.0), axis=1, keepdims=True)
    masks = []
    for r in range(spins):
        column = jnp.where(dil_col == r, 1.0, 0.0)
        masks.append(jnp.broadcast_to(column, (noise_count, depth)).astype(jnp.bfloat16))
    at_lane = lax.broadcasted_iota(jnp.int32, (noise_count, modes), 1)
    at_row = lax.broadcasted_iota(jnp.int32, (noise_count, modes), 0)
    spread = jnp.where(at_lane == at_row + low, jnp.broadcast_to(dil_col, (noise_count, modes)), 0.0)
    dil_lanes = jnp.sum(spread, axis=0, keepdims=True)

    half = spins * low // 128
    per_spin = 2 * half + 1

    def multiply(t, first, end):
        for colour in range(first, end):
            for copy in loads[t * colours + colour]:
                copy.wait()
        span = range(first, end)

        def left(c):
            return jnp.concatenate(
                [left_buf[t, k, :, c].reshape(spins * modes, depth) for k in span], axis=1
            )

        def right_low(c):
            return jnp.concatenate(
                [
                    jnp.concatenate([right_buf[t, k, r, c, :low] for r in range(spins)], axis=0)
                    for k in span
                ],
                axis=1,
            )

        def right_noise(c):
            chosen = []
            for k in span:
                value = right_buf[t, k, 0, c, low:] * masks[0]
                for r in range(1, spins):
                    value = value + right_buf[t, k, r, c, low:] * masks[r]
                chosen.append(value)
            return jnp.concatenate(chosen, axis=1)

        left_re, left_im = left(0), left(1)
        low_re, low_im = right_low(0), right_low(1)
        noise_re, noise_im = right_noise(0), right_noise(1)
        low_out_re = nt_dot(left_re, low_re) + nt_dot(left_im, low_im)
        low_out_im = nt_dot(left_re, low_im) + nt_dot(left_im, -low_re)
        noise_out = nt_dot(left_re, jnp.concatenate([noise_re, noise_im], axis=0)) + nt_dot(
            left_im, jnp.concatenate([noise_im, -noise_re], axis=0)
        )

        def put(k, piece):
            piece = piece.reshape(nxo, nxi, ny, rows, 128)
            if first == 0:
                parts[t, k // kz, k % kz] = piece
            else:
                parts[t, k // kz, k % kz] += piece

        for s in range(spins):
            at = slice(s * modes, (s + 1) * modes)
            for k in range(half):
                put(s * per_spin + k, low_out_re[at, k * 128 : (k + 1) * 128])
                put(s * per_spin + half + k, low_out_im[at, k * 128 : (k + 1) * 128])
            put(s * per_spin + 2 * half, noise_out[at])
        if first == 0:
            for k in range(spins * per_spin, nz * kz):
                parts[t, k // kz, k % kz] = jnp.zeros((nxo, nxi, ny, rows, 128), jnp.float32)

    pending = []

    def send(src, dst, device):
        k = next_sem[0]
        next_sem[0] += 1
        copy = pltpu.make_async_remote_copy(
            src_ref=src, dst_ref=dst, send_sem=send_sem.at[k], recv_sem=recv_sem.at[k],
            device_id=device, device_id_type=MESH,
        )
        copy.start()
        pending.append(copy)
        return copy

    def peer(axis, d):
        if axis == "inner":
            there = (inner + d) % nxi
            return there, {"gx": outer * nxi + there, "gy": gy, "gz": gz}
        if axis == "outer":
            there = (outer + d) % nxo
            return there, {"gx": there * nxi + inner, "gy": gy, "gz": gz}
        if axis == "gy":
            there = (gy + d) % ny
            return there, {"gx": gx, "gy": there, "gz": gz}
        there = (gz + d) % nz
        return there, {"gx": gx, "gy": gy, "gz": there}

    place = {"inner": inner, "outer": outer, "gy": gy, "gz": gz}
    size = {"inner": nxi, "outer": nxo, "gy": ny, "gz": nz}

    def begin(flow):
        axis = flow["order"][flow["step"]]
        at = flow["labels"].index(axis)
        arrivals = flow["bufs"][2 * flow["step"]]
        flow["copies"] = []
        for d in range(1, size[axis]):
            there, device = peer(axis, d)
            index = (slice(None),) * at + (there,)
            flow["copies"].append(send(flow["src"].at[index], arrivals.at[d - 1], device))

    def finish(flow):
        step = flow["step"]
        axis = flow["order"][step]
        at = flow["labels"].index(axis)
        arrivals = flow["bufs"][2 * step]
        total = flow["src"][(slice(None),) * at + (place[axis],)]
        for d, copy in enumerate(flow["copies"]):
            copy.wait_recv()
            total = total + arrivals[d]
        if step < 3:
            result = flow["bufs"][2 * step + 1]
        else:
            result = gathered.at[flow["t"], gz, flow["k0"] : flow["k1"]]
        result[...] = total
        flow["src"] = result
        flow["labels"] = [label for label in flow["labels"] if label != axis]
        flow["step"] = step + 1

    flows = []
    for n, (t, k0, k1, order) in enumerate(flow_specs):
        flows.append({
            "t": t, "k0": k0, "k1": k1, "order": order, "step": 0,
            "src": parts.at[t, :, k0:k1],
            "labels": ["gz", "kz", "outer", "inner", "gy"],
            "bufs": bufs[7 * n : 7 * n + 7],
        })

    def advance(t):
        for flow in flows:
            if flow["t"] != t:
                continue
            if "copies" in flow and flow["step"] < 4:
                finish(flow)
            if flow["step"] < 4:
                begin(flow)
            else:
                mine = gathered.at[t, gz, flow["k0"] : flow["k1"]]
                flow["copies"] = [send(mine, mine, peer("gz", d)[1]) for d in range(1, nz)]

    lane = lax.broadcasted_iota(jnp.int32, (rows, 128), 1)
    is_low = lane < low
    dil = jnp.broadcast_to(dil_lanes, (rows, 128))
    pack = 128 // low
    groups = -(-(2 * gamma_local) // nb)
    width = groups * 128

    def make_fields(t):
        for flow in flows:
            if flow["t"] == t:
                for copy in flow["copies"]:
                    copy.wait_recv()

        def slab(k):
            return gathered[t, k // kz, k % kz]

        for s in range(spins):
            noise = slab(s * per_spin + 2 * half)
            for c in range(2):
                noise_c = noise if c == 1 else pltpu.roll(noise, low, 1)
                for r in range(spins):
                    piece = slab(s * per_spin + c * half + r // pack)
                    if r % pack:
                        piece = pltpu.roll(piece, 128 - (r % pack) * low, 1)
                    blocks[t, s, r, c] = jnp.where(
                        is_low, piece, jnp.where(dil == r, noise_c, 0.0)
                    )

        def one_gamma(g, carry):
            re = jnp.zeros((rows, 128), jnp.float32)
            im = jnp.zeros((rows, 128), jnp.float32)
            for s in range(spins):
                col = cols_ref[s, g]
                phase = phase_ref[s, g]
                block_re = blocks[t, s, col, 0]
                block_im = blocks[t, s, col, 1]
                one = jnp.where(phase == 0, 1.0, jnp.where(phase == 2, -1.0, 0.0))
                eye = jnp.where(phase == 1, 1.0, jnp.where(phase == 3, -1.0, 0.0))
                re = re + (one * block_re - eye * block_im)
                im = im + (one * block_im + eye * block_re)
            fields[t, 0, g] = re
            fields[t, 1, g] = im
            return carry

        lax.fori_loop(0, gammas, one_gamma, 0)

    def send_columns(t):
        picked = []
        for c in range(2):
            for g in range(gamma_local):
                value = fields[t, c, gz * gamma_local + g]
                meson_ref[g, t, c] = value
                picked.append(value)
        while len(picked) % nb:
            picked.append(jnp.zeros((rows, 128), jnp.float32))
        for k in range(groups):
            moved = chunk_transpose(picked[k * nb : (k + 1) * nb], rows)
            for j in range(nb):
                outgoing[t, j, :, k * 128 : (k + 1) * 128] = moved[j]
        columns[t, me] = outgoing[t, me]
        copies = []
        for d in range(1, nb):
            there, device = block_peer(d)
            copies.append(send(outgoing.at[t, there], columns.at[t, me], device))
        return copies

    for k in range(len(CUTS0) - 1):
        multiply(0, CUTS0[k] * colours // 3, CUTS0[k + 1] * colours // 3)
    pl.semaphore_wait(barrier, nb - 1 + nz - 1)
    advance(0)
    for t in range(1, times):
        for k in range(len(CUTS1) - 1):
            multiply(t, CUTS1[k] * colours // 3, CUTS1[k + 1] * colours // 3)
            if t == 1 and k == 0:
                advance(0)
        advance(t)
    done = {0: 2}
    for t in range(1, times):
        done[t] = 1
    arriving = {}
    while len(arriving) < times:
        for t in range(times):
            if done[t] < 5:
                advance(t)
                done[t] += 1
            elif t not in arriving:
                make_fields(t)
                arriving[t] = send_columns(t)

    quarter = gammas * rows
    wide = times * width
    rights = []
    for t in range(times):
        for copy in arriving[t]:
            copy.wait_recv()
        rights.append(columns[t].reshape(nb * rows, width))
    right = jnp.concatenate(rights, axis=1)
    row_w = lax.broadcasted_iota(jnp.int32, (quarter, wide), 0)
    lane_w = lax.broadcasted_iota(jnp.int32, (quarter, wide), 1)
    same = (row_w % rows) == (lane_w % rows)
    per = times * 2 * gamma_local
    src_lane = lax.broadcasted_iota(jnp.int32, (wide, 128), 0)
    dst = lax.broadcasted_iota(jnp.int32, (wide, 128), 1) % per
    src_t = src_lane // width
    src_x = (src_lane % width) // rows
    dst_t = dst // (2 * gamma_local)
    dst_x = dst % (2 * gamma_local)
    swapped = (dst_x + gamma_local) % (2 * gamma_local)
    same_t = src_t == dst_t
    straight = jnp.where(same_t & (src_x == dst_x), 1.0, 0.0)
    crossed = jnp.where(
        same_t & (src_x == swapped), jnp.where(dst_x < gamma_local, -1.0, 1.0), 0.0
    )
    picks = (straight, crossed)
    split = max(1, 128 // (per * times))
    while gammas % split or (gammas // split) % 8:
        split -= 1
    part_rows = gammas // split
    out_lane = lax.broadcasted_iota(jnp.int32, (part_rows, 128), 1) // per
    packed = jnp.zeros((part_rows, 128), jnp.float32)
    sums = [[None] * times, [None] * times]
    for t in range(times):
        for c in range(2):
            left = fields[t, c].reshape(quarter, 128)
            cross = jnp.dot(left, right, precision=EXACT, preferred_element_type=jnp.float32)
            cross = jnp.where(same, cross, 0.0)
            sums[c][t] = jnp.sum(cross.reshape(gammas, rows, wide), axis=1)
    total = jnp.dot(
        jnp.concatenate(sums[0], axis=0), straight, precision=EXACT,
        preferred_element_type=jnp.float32,
    ) + jnp.dot(
        jnp.concatenate(sums[1], axis=0), crossed, precision=EXACT,
        preferred_element_type=jnp.float32,
    )
    for t in range(times):
        for h in range(split):
            piece = total[t * gammas + h * part_rows : t * gammas + (h + 1) * part_rows]
            packed = jnp.where(out_lane == h * times + t, piece, packed)
    totals[me] = packed
    copies = []
    for d in range(1, nb):
        _, device = block_peer(d)
        copies.append(send(totals.at[me], totals.at[me], device))
    for copy in copies:
        copy.wait_recv()
    total = totals[0]
    for j in range(1, nb):
        total = total + totals[j]
    turned = jnp.transpose(total)
    span = times * per
    grid = jnp.concatenate([turned[h * span : (h + 1) * span] for h in range(split)], axis=1)
    for p in range(pairs_ref.shape[1]):
        first, second = pairs_ref[0, p], pairs_ref[1, p]
        for c in range(2):
            value = jnp.zeros((gamma_local, gammas), jnp.float32)
            for t_h in range(times):
                for t_g in range(times):
                    at = ((t_h * times + t_g) * 2 + c) * gamma_local
                    keep = (first == t_g) & (second == t_h)
                    value = value + jnp.where(keep, grid[at : at + gamma_local], 0.0)
            trace_ref[p, c] = value / modes
    for copy in pending:
        copy.wait_send()


def fused(left, right, gamma_cols, gamma_phase, dilution, time_pairs, sizes):
    nx, ny, nz = sizes
    times, spins, parts, colours, modes, depth = left.shape
    nxi = 2 if nx % 2 == 0 else 1
    nxo = nx // nxi
    gammas = gamma_cols.shape[0]
    gamma_local = gammas // nz
    low = modes - dilution.shape[0]
    used = spins * (2 * (spins * low // 128) + 1)
    kz = -(-used // nz)
    rows = modes // (nx * ny)
    nb = nx * ny
    tile = (rows, 128)
    dims = (
        times, spins, colours, low, modes, depth, gammas, gamma_local, nz, kz, nxo, nxi, ny, rows,
    )
    scratch = []
    sems = 0
    for t, k0, k1, order in flow_list(times, kz):
        shapes = []
        left_dims = {"gz": nz, "kz": k1 - k0, "outer": nxo, "inner": nxi, "gy": ny}
        for axis in order:
            n = left_dims.pop(axis)
            sems += n - 1
            rest = tuple(left_dims.values())
            shapes.append((max(n - 1, 1),) + rest + tile)
            shapes.append(rest + tile)
        sems += nz - 1
        scratch += [pltpu.VMEM(shape, jnp.float32) for shape in shapes[:7]]
    sems += (times + 1) * (nb - 1)
    groups = -(-(2 * gamma_local) // nb)
    per = times * 2 * gamma_local
    split = max(1, 128 // (per * times))
    while gammas % split or (gammas // split) % 8:
        split -= 1
    block = (times, colours, spins, parts, modes, depth)
    scratch += [
        pltpu.VMEM(block, jnp.bfloat16),
        pltpu.VMEM(block, jnp.bfloat16),
        pltpu.VMEM((times, nz, kz, nxo, nxi, ny) + tile, jnp.float32),
        pltpu.VMEM((times, nz, kz) + tile, jnp.float32),
        pltpu.VMEM((times, spins, spins, 2) + tile, jnp.float32),
        pltpu.VMEM((times, 2, gammas) + tile, jnp.float32),
        pltpu.VMEM((times, nb, rows, groups * 128), jnp.float32),
        pltpu.VMEM((times, nb, rows, groups * 128), jnp.float32),
        pltpu.VMEM((nb, gammas // split, 128), jnp.float32),
        pltpu.SemaphoreType.DMA((2 * times * colours,)),
        pltpu.SemaphoreType.DMA((sems,)),
        pltpu.SemaphoreType.DMA((sems,)),
    ]
    vmem = pl.BlockSpec(memory_space=pltpu.VMEM)
    smem = pl.BlockSpec(memory_space=pltpu.SMEM)
    hbm = pl.BlockSpec(memory_space=pl.ANY)
    return pl.pallas_call(
        functools.partial(fused_kernel, dims),
        in_specs=[smem, smem, smem, vmem, hbm, hbm],
        out_specs=[vmem, vmem],
        out_shape=[
            jax.ShapeDtypeStruct((gamma_local, times, 2) + tile, jnp.float32),
            jax.ShapeDtypeStruct((time_pairs.shape[0], 2, gamma_local, gammas), jnp.float32),
        ],
        scratch_shapes=scratch,
        compiler_params=pltpu.CompilerParams(
            collective_id=0, has_side_effects=True, vmem_limit_bytes=54 * 1024 * 1024
        ),
        name="meson_fields",
    )(gamma_cols.T, gamma_phase.T, time_pairs.T, dilution.reshape(1, -1), left, right)


def local(sizes, left_modes, right_modes, gamma_cols, gamma_phase, dilution, time_pairs):
    left = jnp.transpose(left_modes, (0, 1, 2, 4, 3, 5))
    right = jnp.transpose(right_modes, (0, 1, 2, 4, 3, 5))
    meson_fields, traces = fused(
        left, right, gamma_cols, gamma_phase, dilution, time_pairs, sizes
    )
    return (meson_fields, jnp.transpose(traces, (0, 2, 3, 1)))


def solution(mesh):
    sizes = (mesh.shape["gx"], mesh.shape["gy"], mesh.shape["gz"])
    modes_spec = P(None, None, None, None, None, ("gx", "gy", "gz"))
    return jax.shard_map(
        functools.partial(local, sizes),
        mesh=mesh,
        in_specs=(modes_spec, modes_spec, P(), P(), P(), P()),
        out_specs=(P("gz", None, None, ("gx", "gy"), None), P(None, "gz", None, None)),
        check_vma=False,
    )
```
